32 devices in a mesh: row: 4 (over y, x), col: 8 (over z, core).
Axes of the slice: x: 2, y: 2, z: 4, core: 2. Of those that a mesh axis runs over, the one named last changes fastest.
Arguments:
- pair: float32 [256, 256, 128], P('row', 'col'), may hold values from -6 to 6
- valid_length: int32 [1], replicated, may hold values from 64 to 255
- tri_in: bfloat16 [128, 512], replicated, may hold values from -0.5 to 0.5
- tri_gate: bfloat16 [128, 128], replicated, may hold values from -0.5 to 0.5
- tri_out: bfloat16 [128, 128], replicated, may hold values from -0.5 to 0.5
- att_in: bfloat16 [128, 512], replicated, may hold values from -16.9705627 to 16.9705627
- att_bias: bfloat16 [128, 4], replicated, may hold values from -0.5 to 0.5
- att_out: bfloat16 [128, 128], replicated, may hold values from -0.5 to 0.5
Outputs:
- pair_out: float32 [256, 256, 128], P('row', 'col')
The draws below stay inside these ranges and needn't reach their ends.
Inputs may be any that keep to these rules, and one draw needn't show every extreme that they name: Tokens at positions below valid_length[0] are real, the rest are padding.
All inputs are finite; a program needn't handle non-finite values.
Results may differ from the reference program's by a relative error of at most 0.025.
Values may be sent and summed in bfloat16 or wider, within the bound.
A program may use at most 128 MiB of HBM per device.

```python
import jax
import jax.numpy as jnp
from jax import lax

C = 128
CH = 128
H = 4
DH = 32
N = 256


def draw_att_in(key, part):
    raw = jax.random.truncated_normal(key, -4.0, 4.0, (C, 4 * C), jnp.float32) * C ** (-0.5)
    return raw.astype(jnp.bfloat16)


def shard_levels(stream_key, dims, shards, least, largest):
    factor_of, own = 1.0, jax.random.fold_in(stream_key, 6)
    for dim, shards_of in shards:
        heights = jnp.exp(jax.random.uniform(jax.random.fold_in(own, dim), (shards_of,), jnp.float32, least / len(shards), largest / len(shards)))
        factor_of = factor_of * jnp.repeat(heights, dims[dim] // shards_of).reshape([-1 if axis == dim else 1 for axis in range(len(dims))])
    return factor_of


def noise(key, extent, width, most, shards=(), held_as=jnp.bfloat16):
    array = width * jax.random.normal(key, extent, jnp.float32)
    if shards:
        array = array * shard_levels(key, extent, shards, -0.22, 0.18)
    return jnp.clip(array, -most, most).astype(held_as)


def setup_inputs(seed: int = 0) -> dict:
    splits = jax.random.split(jax.random.key(seed), 9)
    return {
        "pair": noise(splits[0], (N, N, C), 1.0, 6.0, ((0, 4), (1, 8)), jnp.float32),
        "valid_length": jax.random.randint(splits[1], (1,), N // 4, N).astype(jnp.int32),
        "tri_in": noise(splits[2], (C, 4 * CH), C ** -0.5, 0.5),
        "tri_gate": noise(splits[3], (C, C), C ** -0.5, 0.5),
        "tri_out": noise(splits[4], (CH, C), CH ** -0.5, 0.5),
        "att_in": draw_att_in(jax.random.fold_in(splits[8], 71), 0),
        "att_bias": noise(splits[6], (C, H), C ** -0.5, 0.5),
        "att_out": noise(splits[7], (C, C), C ** -0.5, 0.5),
    }


def layer_norm(values):
    center = values - lax.optimization_barrier(jnp.mean(values, axis=-1, keepdims=True))
    return center * lax.rsqrt(lax.optimization_barrier(jnp.mean(center * center, axis=-1, keepdims=True)) + 1e-05)

def reference(pair, valid_length, tri_in, tri_gate, tri_out, att_in, att_bias, att_out):
    tokens = jnp.arange(N).astype(jnp.int32)
    keep = (tokens < valid_length[0]).astype(jnp.float32)
    blocks = N // 8
    normed_pair = layer_norm(pair).astype(jnp.bfloat16)

    def edges(packed):
        rows, row_keep = packed
        projected = jnp.dot(rows, tri_in, preferred_element_type=jnp.float32)
        weight = (row_keep[:, None] * keep[None, :])[:, :, None]
        left = jax.nn.sigmoid(projected[..., :CH]) * projected[..., CH:2 * CH] * weight
        right = jax.nn.sigmoid(projected[..., 2 * CH:3 * CH]) * projected[..., 3 * CH:] * weight
        return (left.astype(jnp.bfloat16), right.astype(jnp.bfloat16))
    left_edges, right_edges = lax.map(edges, (normed_pair.reshape(blocks, 8, N, C), keep.reshape(blocks, 8)))
    left_edges = left_edges.reshape(N, N, CH)
    right_edges = right_edges.reshape(N, N, CH)
    products = jnp.einsum('ikc,jkc->ijc', left_edges.astype(jnp.float32), right_edges.astype(jnp.float32))
    normed_products = layer_norm(products).astype(jnp.bfloat16)
    update = jax.nn.sigmoid(jnp.dot(normed_pair, tri_gate, preferred_element_type=jnp.float32)) * jnp.dot(normed_products, tri_out, preferred_element_type=jnp.float32)
    middle = pair + update
    normed_mid = layer_norm(middle).astype(jnp.bfloat16)
    bias_all = jnp.dot(normed_mid, att_bias, preferred_element_type=jnp.float32).astype(jnp.bfloat16)
    bias_heads = jnp.transpose(bias_all.astype(jnp.float32), (2, 0, 1))
    mask_bias = jnp.where(tokens < valid_length[0], 0.0, -1000000000.0).astype(jnp.float32)

    def attend(packed):
        block_mid, block_norm = packed
        projected = jnp.dot(block_norm, att_in, preferred_element_type=jnp.float32)
        query = (projected[..., :C] * DH ** (-0.5)).astype(jnp.bfloat16).reshape(8, N, H, DH)
        keys = projected[..., C:2 * C].astype(jnp.bfloat16).reshape(8, N, H, DH)
        values = projected[..., 2 * C:3 * C].astype(jnp.bfloat16).reshape(8, N, H, DH)
        gate = jax.nn.sigmoid(projected[..., 3 * C:])
        scores = jnp.einsum('ijhd,ikhd->ihjk', query.astype(jnp.float32), keys.astype(jnp.float32))
        scores = scores + bias_heads[None] + mask_bias[None, None, None, :]
        weights = jax.nn.softmax(scores, axis=-1)
        attended = jnp.einsum('ihjk,ikhd->ijhd', weights, values.astype(jnp.float32)).reshape(8, N, C)
        gated = (gate * attended).astype(jnp.bfloat16)
        return block_mid + jnp.dot(gated, att_out, preferred_element_type=jnp.float32)
    result = lax.map(attend, (middle.reshape(blocks, 8, N, C), normed_mid.reshape(blocks, 8, N, C)))
    return result.reshape(N, N, C)
```

```python
import functools

import jax
import jax.numpy as jnp
from jax import lax
from jax.experimental import pallas as pl
from jax.experimental.pallas import tpu as pltpu
from jax.sharding import PartitionSpec as P

MESH = pl.DeviceIdType.MESH
F32 = jnp.float32
BF16 = jnp.bfloat16


def norm(values, axis):
    center = values - jnp.mean(values, axis=axis, keepdims=True)
    return center * lax.rsqrt(jnp.mean(center * center, axis=axis, keepdims=True) + 1e-05)


def swap_groups(blocks, lane, group):
    count = len(blocks)
    width = count * group
    out = []
    for b in range(count):
        total = None
        for a in range(count):
            shift = (group * (a - b)) % width
            moved = blocks[a] if shift == 0 else pltpu.roll(blocks[a], shift, 1)
            total = moved if total is None else jnp.where(lane == a, moved, total)
        out.append(total)
    return out


def kernel(
    dims,
    pair_ref, keep_ref, mask_ref, tri_in_ref, tri_gate_ref, tri_out_ref, att_in_ref, bias_w_ref,
    middle_ref, gated_ref,
    edge_f, edge_send, edge_recv, left_s, right_s, prod_send, prod_recv, prod_f,
    mid_send, mid_recv, qkv_s, gate_s, bias_f, bias_send, bias_recv, bias_full, gated_s,
    send1, recv1, send2, recv2, send3, recv3, send4, recv4, send5, recv5,
):
    nrow, ncol, rows_dev, cols_dev, width, heads = dims
    ndev = nrow * ncol
    total = ncol * cols_dev
    group = 128 // cols_dev
    tiles = rows_dev // group
    chans = width // ndev
    per = rows_dev // ncol
    head_size = width // heads
    my_row, my_col = lax.axis_index("row"), lax.axis_index("col")
    me = my_row * ncol + my_col

    def other(step):
        peer = lax.rem(me + step, ndev)
        return peer, (peer // ncol, lax.rem(peer, ncol))

    barrier = pltpu.get_barrier_semaphore()

    def greet(step, carry):
        pl.semaphore_signal(barrier, inc=1, device_id=other(step)[1], device_id_type=MESH)
        return carry

    lax.fori_loop(1, ndev, greet, 0)

    for t in range(tiles):
        rows = jnp.concatenate([pair_ref[g * tiles + t] for g in range(group)], axis=0)
        normed = norm(rows, 1).astype(BF16)
        proj = jnp.dot(normed, tri_in_ref[...], preferred_element_type=F32)
        keep = keep_ref[pl.ds(t, 1), :]
        left = jax.nn.sigmoid(proj[:, :width]) * proj[:, width : 2 * width]
        right = jax.nn.sigmoid(proj[:, 2 * width : 3 * width]) * proj[:, 3 * width :]
        edge_f[pl.ds(t, width, stride=2 * tiles), :] = jnp.transpose(left) * keep
        edge_f[pl.ds(tiles + t, width, stride=2 * tiles), :] = jnp.transpose(right) * keep
    span = chans * 2 * tiles
    for d in range(ndev):
        edge_send[d] = edge_f[pl.ds(d * span, span), :].astype(BF16)
    pl.semaphore_wait(barrier, ndev - 1)

    def exchange(source, target, sends, recvs):
        def make(step):
            peer, where = other(step)
            return pltpu.make_async_remote_copy(
                src_ref=source(peer), dst_ref=target, send_sem=sends.at[step],
                recv_sem=recvs.at[step], device_id=where, device_id_type=MESH,
            )

        def begin(step, carry):
            make(step).start()
            return carry

        def finish(step, carry):
            make(step).wait()
            return carry

        return (
            lambda: lax.fori_loop(1, ndev, begin, 0),
            lambda: lax.fori_loop(1, ndev, finish, 0),
        )

    start, wait = exchange(lambda d: edge_send.at[d], edge_recv.at[me], send1, recv1)
    start()
    edge_recv[me] = edge_send[me]
    wait()

    lane = lax.broadcasted_iota(jnp.int32, (tiles, 128), 1) // cols_dev
    for c in range(chans):
        for side, operand in ((0, left_s), (1, right_s)):
            first = (c * 2 + side) * tiles
            for r in range(nrow):
                for half in range(ncol // group):
                    blocks = [
                        edge_recv[r * ncol + half * group + a, first : first + tiles, :].astype(F32)
                        for a in range(group)
                    ]
                    for b, piece in enumerate(swap_groups(blocks, lane, cols_dev)):
                        operand[
                            pl.ds(r * rows_dev + b * tiles, tiles), pl.ds(half * 128, 128)
                        ] = piece.astype(BF16)
        products = lax.dot_general(
            left_s[...], right_s[...], (((1,), (1,)), ((), ())), preferred_element_type=F32
        )
        for r in range(nrow):
            for half in range(ncol // group):
                blocks = [
                    products[
                        r * rows_dev + a * tiles : r * rows_dev + (a + 1) * tiles,
                        half * 128 : (half + 1) * 128,
                    ]
                    for a in range(group)
                ]
                for b, piece in enumerate(swap_groups(blocks, lane, cols_dev)):
                    prod_send[
                        r * ncol + half * group + b, pl.ds(c * tiles, tiles), :
                    ] = piece.astype(BF16)

    start, wait = exchange(lambda d: prod_send.at[d], prod_recv.at[me], send2, recv2)
    start()
    prod_recv[me] = prod_send[me]
    wait()

    span = chans * tiles
    for d in range(ndev):
        prod_f[pl.ds(d * span, span), :] = prod_recv[d].astype(F32)
    for t in range(tiles):
        prods = norm(prod_f[pl.ds(t, width, stride=tiles), :], 0)
        prods = jnp.transpose(prods).astype(BF16)
        update = jnp.dot(prods, tri_out_ref[...], preferred_element_type=F32)
        rows = jnp.concatenate([pair_ref[g * tiles + t] for g in range(group)], axis=0)
        normed = norm(rows, 1).astype(BF16)
        gate = jax.nn.sigmoid(jnp.dot(normed, tri_gate_ref[...], preferred_element_type=F32))
        middle = rows + gate * update
        normed_mid = norm(middle, 1).astype(BF16)
        for g in range(group):
            i = g * tiles + t
            middle_ref[i] = middle[g * cols_dev : (g + 1) * cols_dev]
            mid_send[i // per, i % per] = normed_mid[g * cols_dev : (g + 1) * cols_dev]

    mine = pl.ds(pl.multiple_of(my_col * cols_dev, cols_dev), cols_dev)

    def mid_copy(step):
        peer = lax.rem(my_col + step, ncol)
        return pltpu.make_async_remote_copy(
            src_ref=mid_send.at[peer], dst_ref=mid_recv.at[:, mine, :], send_sem=send3.at[step],
            recv_sem=recv3.at[step], device_id=(my_row, peer), device_id_type=MESH,
        )

    for step in range(1, ncol):
        mid_copy(step).start()
    mid_recv[:, mine, :] = mid_send[my_col]
    for step in range(1, ncol):
        mid_copy(step).wait()

    for i in range(per):
        own = lax.dot_general(
            bias_w_ref[...], mid_recv[i], (((1,), (1,)), ((), ())), preferred_element_type=F32
        )
        for h in range(heads):
            bias_f[pl.ds(h * per + i, 1), :] = own[h : h + 1]
    bias_send[...] = bias_f[...].astype(BF16)
    start, wait = exchange(lambda d: bias_send, bias_recv.at[me], send4, recv4)
    start()
    bias_recv[me] = bias_send[...]
    for i in range(per):
        proj = jnp.dot(mid_recv[i], att_in_ref[...], preferred_element_type=F32)
        qkv_s[i, :, :width] = (proj[:, :width] * head_size ** (-0.5)).astype(BF16)
        qkv_s[i, :, width : 3 * width] = proj[:, width : 3 * width].astype(BF16)
        gate_s[i] = jax.nn.sigmoid(proj[:, 3 * width :])
    wait()
    mask = mask_ref[...]
    for d in range(ndev):
        piece = bias_recv[d].astype(F32) + mask
        for h in range(heads):
            bias_full[h, pl.ds(d * per, per), :] = piece[h * per : (h + 1) * per]

    head = lax.broadcasted_iota(jnp.int32, (total, width), 1) // head_size

    def home_copy(i, step):
        peer = lax.rem(my_col + step, ncol)
        theirs = pl.ds(pl.multiple_of(peer * cols_dev, cols_dev), cols_dev)
        return pltpu.make_async_remote_copy(
            src_ref=gated_s.at[i, theirs, :], dst_ref=gated_ref.at[my_col * per + i],
            send_sem=send5.at[i, step], recv_sem=recv5.at[i, step],
            device_id=(my_row, peer), device_id_type=MESH,
        )

    def attend(i, carry):
        query = qkv_s[i, :, :width]
        keys = qkv_s[i, :, width : 2 * width]
        values = jnp.concatenate(
            [qkv_s[i, :, 2 * width : 3 * width], jnp.ones((total, width), BF16)], axis=1
        )
        joined = jnp.zeros((total, width), F32)
        for h in range(heads):
            scores = lax.dot_general(
                jnp.where(head == h, query, jnp.zeros_like(query)), keys,
                (((1,), (1,)), ((), ())), preferred_element_type=F32,
            )
            scores = scores + bias_full[h]
            expo = jnp.exp(scores - jnp.max(scores, axis=1, keepdims=True)).astype(BF16)
            both = jnp.dot(expo, values, preferred_element_type=F32)
            joined = jnp.where(head == h, both[:, :width] / both[:, width:], joined)
        gated_s[i] = (gate_s[i] * joined).astype(BF16)
        for step in range(1, ncol):
            home_copy(i, step).start()
        gated_ref[my_col * per + i] = gated_s[i, mine, :]
        return carry

    lax.fori_loop(0, per, attend, 0)

    def finish(i, carry):
        for step in range(1, ncol):
            home_copy(i, step).wait()
        return carry

    lax.fori_loop(0, per, finish, 0)


def per_device(pair, valid_length, tri_in, tri_gate, tri_out, att_in, att_bias, att_out):
    rows_dev, cols_dev, width = pair.shape
    heads = att_bias.shape[1]
    nrow, ncol = lax.axis_size("row"), lax.axis_size("col")
    ndev = nrow * ncol
    total = ncol * cols_dev
    group = 128 // cols_dev
    tiles = rows_dev // group
    chans = width // ndev
    per = rows_dev // ncol
    row_ids = lax.axis_index("row") * rows_dev + jnp.arange(rows_dev)
    col_ids = lax.axis_index("col") * cols_dev + jnp.arange(cols_dev)
    keep = ((row_ids < valid_length[0])[:, None] & (col_ids < valid_length[0])[None, :]).astype(F32)
    keep = keep.reshape(group, tiles, cols_dev).transpose(1, 0, 2).reshape(tiles, 128)
    mask = jnp.where(jnp.arange(total) < valid_length[0], 0.0, -1000000000.0).astype(F32)[None]
    bias_w = jnp.pad(att_bias.T, ((0, 16 - heads), (0, 0)))
    vmem = pl.BlockSpec(memory_space=pltpu.VMEM)
    dma = pltpu.SemaphoreType.DMA
    middle, gated = pl.pallas_call(
        functools.partial(kernel, (nrow, ncol, rows_dev, cols_dev, width, heads)),
        out_shape=(
            jax.ShapeDtypeStruct((rows_dev, cols_dev, width), F32),
            jax.ShapeDtypeStruct((rows_dev, cols_dev, width), BF16),
        ),
        in_specs=[vmem] * 8,
        out_specs=(vmem, vmem),
        scratch_shapes=[
            pltpu.VMEM((width * 2 * tiles, 128), F32),
            pltpu.VMEM((ndev, chans * 2 * tiles, 128), BF16),
            pltpu.VMEM((ndev, chans * 2 * tiles, 128), BF16),
            pltpu.VMEM((total, total), BF16),
            pltpu.VMEM((total, total), BF16),
            pltpu.VMEM((ndev, chans * tiles, 128), BF16),
            pltpu.VMEM((ndev, chans * tiles, 128), BF16),
            pltpu.VMEM((width * tiles, 128), F32),
            pltpu.VMEM((ncol, per, cols_dev, width), BF16),
            pltpu.VMEM((per, total, width), BF16),
            pltpu.VMEM((per, total, 3 * width), BF16),
            pltpu.VMEM((per, total, width), F32),
            pltpu.VMEM((heads * per, total), F32),
            pltpu.VMEM((heads * per, total), BF16),
            pltpu.VMEM((ndev, heads * per, total), BF16),
            pltpu.VMEM((heads, total, total), F32),
            pltpu.VMEM((per, total, width), BF16),
            dma((ndev,)), dma((ndev,)), dma((ndev,)), dma((ndev,)),
            dma((ncol,)), dma((ncol,)), dma((ndev,)), dma((ndev,)),
            dma((per, ncol)), dma((per, ncol)),
        ],
        compiler_params=pltpu.CompilerParams(
            collective_id=0, has_side_effects=True, vmem_limit_bytes=56 * 1024 * 1024
        ),
    )(pair, keep, mask, tri_in, tri_gate, tri_out, att_in, bias_w)
    return middle + jnp.dot(gated, att_out, preferred_element_type=F32)


def solution(mesh):
    placed = (P("row", "col", None), P(), P(), P(), P(), P(), P(), P())
    return jax.shard_map(
        per_device, mesh=mesh, in_specs=placed, out_specs=P("row", "col", None), check_vma=False
    )
```

```python
import functools

import jax
import jax.numpy as jnp
from jax import lax
from jax.experimental import pallas as pl
from jax.experimental.pallas import tpu as pltpu
from jax.sharding import PartitionSpec as P

MESH = pl.DeviceIdType.MESH
F32 = jnp.float32
BF16 = jnp.bfloat16


def norm(values, axis):
    center = values - jnp.mean(values, axis=axis, keepdims=True)
    return center * lax.rsqrt(jnp.mean(center * center, axis=axis, keepdims=True) + 1e-05)


def swap_groups(blocks, lane, group):
    count = len(blocks)
    width = count * group
    out = []
    for b in range(count):
        total = None
        for a in range(count):
            shift = (group * (a - b)) % width
            moved = blocks[a] if shift == 0 else pltpu.roll(blocks[a], shift, 1)
            total = moved if total is None else jnp.where(lane == a, moved, total)
        out.append(total)
    return out


def kernel(
    dims,
    valid_ref, pair_ref, tri_in_ref, tri_gate_ref, tri_out_ref, att_in_ref, bias_w_ref, att_out_ref,
    out_ref,
    normed_s, edge_f, left_send, right_send, left_recv, right_recv, left_s, right_s,
    prod_send, prod_recv, prod_f, tri_gate_s, mid_send, mid_recv, qkv_s, gate_s,
    bias_f, bias_send, bias_recv, bias_full, gated_s, gated_recv,
    send_l, recv_l, send_r, recv_r, send_p, recv_p, send_m, recv_m, send_b, recv_b, send_c, recv_c,
    send_g, recv_g,
):
    nrow, ncol, rows_dev, cols_dev, width, heads = dims
    ndev = nrow * ncol
    total = ncol * cols_dev
    group = 128 // cols_dev
    tiles = rows_dev // group
    chans = width // ndev
    parts = 2 if chans % 2 == 0 else 1
    each = chans // parts
    per = rows_dev // ncol
    head_size = width // heads
    my_row, my_col = lax.axis_index("row"), lax.axis_index("col")
    me = my_row * ncol + my_col
    valid = valid_ref[0]

    def other(step):
        peer = lax.rem(me + step, ndev)
        return peer, (peer // ncol, lax.rem(peer, ncol))

    def loop(count, act):
        def run(step, carry):
            act(step)
            return carry

        lax.fori_loop(1, count, run, 0)

    barrier = pltpu.get_barrier_semaphore()
    loop(
        ndev,
        lambda step: pl.semaphore_signal(
            barrier, inc=1, device_id=other(step)[1], device_id_type=MESH
        ),
    )

    lanes = lax.broadcasted_iota(jnp.int32, (1, 128), 1)
    lane_col = my_col * cols_dev + lanes % cols_dev
    lane_row = my_row * rows_dev + (lanes // cols_dev) * tiles

    def edges(side):
        first = 2 * side * width
        for t in range(tiles):
            if side == 0:
                rows = jnp.concatenate([pair_ref[g * tiles + t] for g in range(group)], axis=0)
                normed_s[t] = norm(rows, 1).astype(BF16)
            proj = jnp.dot(
                normed_s[t], tri_in_ref[:, first : first + 2 * width], preferred_element_type=F32
            )
            keep = jnp.where((lane_row + t < valid) & (lane_col < valid), 1.0, 0.0)
            edge = jax.nn.sigmoid(proj[:, :width]) * proj[:, width:]
            edge_f[side, pl.ds(t, width, stride=tiles), :] = jnp.transpose(edge) * keep

    def pack(side, target):
        for c in range(chans):
            target[c] = edge_f[side, pl.ds(c * ndev * tiles, ndev * tiles), :].astype(BF16)

    def share(peer):
        return pl.ds(pl.multiple_of(peer * tiles, tiles), tiles)

    def left_copy(step):
        peer, where = other(step)
        return pltpu.make_async_remote_copy(
            src_ref=left_send.at[:, share(peer), :], dst_ref=left_recv.at[me],
            send_sem=send_l.at[step], recv_sem=recv_l.at[step],
            device_id=where, device_id_type=MESH,
        )

    def right_copy(part, step):
        peer, where = other(step)
        some = pl.ds(part * each, each)
        return pltpu.make_async_remote_copy(
            src_ref=right_send.at[some, share(peer), :], dst_ref=right_recv.at[me, some],
            send_sem=send_r.at[part, step], recv_sem=recv_r.at[part, step],
            device_id=where, device_id_type=MESH,
        )

    edges(0)
    pack(0, left_send)
    pl.semaphore_wait(barrier, ndev - 1)
    loop(ndev, lambda step: left_copy(step).start())
    edges(1)
    pack(1, right_send)
    for part in range(parts):
        loop(ndev, lambda step: right_copy(part, step).start())
    left_recv[me] = left_send[:, share(me), :]
    right_recv[me] = right_send[:, share(me), :]
    for t in range(tiles):
        tri_gate_s[t] = jax.nn.sigmoid(
            jnp.dot(normed_s[t], tri_gate_ref[...], preferred_element_type=F32)
        )
    loop(ndev, lambda step: left_copy(step).wait())

    lane = lax.broadcasted_iota(jnp.int32, (tiles, 128), 1) // cols_dev

    def spread(c, source, operand):
        for r in range(nrow):
            for half in range(ncol // group):
                blocks = [
                    source[r * ncol + half * group + a, c].astype(F32) for a in range(group)
                ]
                for b, piece in enumerate(swap_groups(blocks, lane, cols_dev)):
                    operand[
                        pl.ds(r * rows_dev + b * tiles, tiles), pl.ds(half * 128, 128)
                    ] = piece.astype(BF16)

    def prod_copy(part, step):
        peer, where = other(step)
        some = pl.ds(part * each, each)
        return pltpu.make_async_remote_copy(
            src_ref=prod_send.at[peer, some], dst_ref=prod_recv.at[me, some],
            send_sem=send_p.at[part, step], recv_sem=recv_p.at[part, step],
            device_id=where, device_id_type=MESH,
        )

    for c in range(chans):
        spread(c, left_recv, left_s.at[c])
    for part in range(parts):
        loop(ndev, lambda step: right_copy(part, step).wait())
        for c in range(part * each, (part + 1) * each):
            spread(c, right_recv, right_s.at[c])
            products = lax.dot_general(
                left_s[c], right_s[c], (((1,), (1,)), ((), ())), preferred_element_type=F32
            )
            for r in range(nrow):
                for half in range(ncol // group):
                    blocks = [
                        products[
                            r * rows_dev + a * tiles : r * rows_dev + (a + 1) * tiles,
                            half * 128 : (half + 1) * 128,
                        ]
                        for a in range(group)
                    ]
                    for b, piece in enumerate(swap_groups(blocks, lane, cols_dev)):
                        prod_send[r * ncol + half * group + b, c] = piece.astype(BF16)
        loop(ndev, lambda step: prod_copy(part, step).start())
    prod_recv[me] = prod_send[me]

    for part in range(parts):
        loop(ndev, lambda step: prod_copy(part, step).wait())
        for c in range(part * each, (part + 1) * each):
            for d in range(ndev):
                prod_f[pl.ds((c * ndev + d) * tiles, tiles), :] = prod_recv[d, c].astype(F32)

    def strip(peer):
        return pl.ds(pl.multiple_of(peer * cols_dev, cols_dev), cols_dev)

    def mid_copy(i, step):
        peer = lax.rem(my_col + step, ncol)
        return pltpu.make_async_remote_copy(
            src_ref=mid_send.at[i, peer], dst_ref=mid_recv.at[i, strip(my_col), :],
            send_sem=send_m.at[i, step], recv_sem=recv_m.at[i, step],
            device_id=(my_row, peer), device_id_type=MESH,
        )

    for i in range(per):
        for t in range(i, tiles, per):
            prods = norm(prod_f[pl.ds(t, width, stride=tiles), :], 0)
            prods = jnp.transpose(prods).astype(BF16)
            update = jnp.dot(prods, tri_out_ref[...], preferred_element_type=F32)
            rows = jnp.concatenate([pair_ref[g * tiles + t] for g in range(group)], axis=0)
            middle = rows + tri_gate_s[t] * update
            normed_mid = norm(middle, 1).astype(BF16)
            for g in range(group):
                row = g * tiles + t
                out_ref[row] = middle[g * cols_dev : (g + 1) * cols_dev]
                mid_send[i, row // per] = normed_mid[g * cols_dev : (g + 1) * cols_dev]
        for step in range(1, ncol):
            mid_copy(i, step).start()
        mid_recv[i, strip(my_col), :] = mid_send[i, my_col]

    for i in range(per):
        for step in range(1, ncol):
            mid_copy(i, step).wait()
        own = lax.dot_general(
            bias_w_ref[...], mid_recv[i], (((0,), (1,)), ((), ())), preferred_element_type=F32
        )
        for h in range(heads):
            bias_f[pl.ds(h * per + i, 1), :] = own[h : h + 1]
        if i < per - 1:
            project(i, mid_recv, att_in_ref, qkv_s, gate_s, width, head_size)
    bias_send[...] = bias_f[...].astype(BF16)

    side = lax.rem(my_col, 2)
    mine = me // 2

    def bias_copy(step):
        peer = 2 * lax.rem(mine + step, ndev // 2) + side
        return pltpu.make_async_remote_copy(
            src_ref=bias_send, dst_ref=bias_recv.at[side, mine],
            send_sem=send_b.at[step], recv_sem=recv_b.at[step],
            device_id=(peer // ncol, lax.rem(peer, ncol)), device_id_type=MESH,
        )

    loop(ndev // 2, lambda step: bias_copy(step).start())
    bias_recv[side, mine] = bias_send[...]
    project(per - 1, mid_recv, att_in_ref, qkv_s, gate_s, width, head_size)
    loop(ndev // 2, lambda step: bias_copy(step).wait())
    hand = pltpu.make_async_remote_copy(
        src_ref=bias_recv.at[side], dst_ref=bias_recv.at[side],
        send_sem=send_c, recv_sem=recv_c,
        device_id=(my_row, my_col + 1 - 2 * side), device_id_type=MESH,
    )
    hand.start()
    hand.wait()
    tokens = lax.broadcasted_iota(jnp.int32, (1, total), 1)
    mask = jnp.where(tokens < valid, 0.0, -1000000000.0)
    for d in range(ndev):
        piece = bias_recv[d % 2, d // 2].astype(F32) + mask
        for h in range(heads):
            bias_full[h, pl.ds(d * per, per), :] = piece[h * per : (h + 1) * per]

    block = 128
    head = lax.broadcasted_iota(jnp.int32, (block, width), 1) // head_size

    def home_copy(i, step):
        peer = lax.rem(my_col + step, ncol)
        return pltpu.make_async_remote_copy(
            src_ref=gated_s.at[i, strip(peer), :], dst_ref=gated_recv.at[i, strip(my_col), :],
            send_sem=send_g.at[i, step], recv_sem=recv_g.at[i, step],
            device_id=(my_row, peer), device_id_type=MESH,
        )

    def attend(i, carry):
        keys = qkv_s[i, :, width : 2 * width]
        values = jnp.concatenate(
            [qkv_s[i, :, 2 * width : 3 * width], jnp.ones((total, width), BF16)], axis=1
        )
        for first in range(0, total, block):
            query = qkv_s[i, first : first + block, :width]
            top = jnp.zeros((block, width), F32)
            bottom = jnp.ones((block, width), F32)
            for h in range(heads):
                scores = lax.dot_general(
                    jnp.where(head == h, query, jnp.zeros_like(query)), keys,
                    (((1,), (1,)), ((), ())), preferred_element_type=F32,
                )
                scores = scores + bias_full[h, first : first + block, :]
                expo = jnp.exp(scores - jnp.max(scores, axis=1, keepdims=True)).astype(BF16)
                both = jnp.dot(expo, values, preferred_element_type=F32)
                top = jnp.where(head == h, both[:, :width], top)
                bottom = jnp.where(head == h, both[:, width:], bottom)
            gated_s[i, first : first + block, :] = (
                gate_s[i, first : first + block, :] * top / bottom
            ).astype(BF16)
        for step in range(1, ncol):
            home_copy(i, step).start()
        gated_recv[i, strip(my_col), :] = gated_s[i, strip(my_col), :]
        return carry

    lax.fori_loop(0, per, attend, 0)

    def finish(i, carry):
        for step in range(1, ncol):
            home_copy(i, step).wait()
        added = jnp.dot(gated_recv[i], att_out_ref[...], preferred_element_type=F32)
        for q in range(ncol):
            out_ref[q * per + i] += added[q * cols_dev : (q + 1) * cols_dev]
        return carry

    lax.fori_loop(0, per, finish, 0)


def project(i, mid_recv, att_in_ref, qkv_s, gate_s, width, head_size):
    proj = jnp.dot(mid_recv[i], att_in_ref[...], preferred_element_type=F32)
    qkv_s[i, :, :width] = (proj[:, :width] * head_size ** (-0.5)).astype(BF16)
    qkv_s[i, :, width : 3 * width] = proj[:, width : 3 * width].astype(BF16)
    gate_s[i] = jax.nn.sigmoid(proj[:, 3 * width :])


def per_device(pair, valid_length, tri_in, tri_gate, tri_out, att_in, att_bias, att_out):
    rows_dev, cols_dev, width = pair.shape
    heads = att_bias.shape[1]
    nrow, ncol = lax.axis_size("row"), lax.axis_size("col")
    ndev = nrow * ncol
    total = ncol * cols_dev
    tiles = rows_dev // (128 // cols_dev)
    chans = width // ndev
    parts = 2 if chans % 2 == 0 else 1
    per = rows_dev // ncol
    vmem = pl.BlockSpec(memory_space=pltpu.VMEM)
    sems = lambda *shape: [pltpu.SemaphoreType.DMA(shape)] * 2
    held = lambda dtype, *shape: pltpu.VMEM(shape, dtype)
    return pl.pallas_call(
        functools.partial(kernel, (nrow, ncol, rows_dev, cols_dev, width, heads)),
        out_shape=jax.ShapeDtypeStruct((rows_dev, cols_dev, width), F32),
        in_specs=[pl.BlockSpec(memory_space=pltpu.SMEM)] + [vmem] * 7,
        out_specs=vmem,
        scratch_shapes=[
            held(BF16, tiles, 128, width),
            held(F32, 2, width * tiles, 128),
            held(BF16, chans, ndev * tiles, 128),
            held(BF16, chans, ndev * tiles, 128),
            held(BF16, ndev, chans, tiles, 128),
            held(BF16, ndev, chans, tiles, 128),
            held(BF16, chans, total, total),
            held(BF16, chans, total, total),
            held(BF16, ndev, chans, tiles, 128),
            held(BF16, ndev, chans, tiles, 128),
            held(F32, width * tiles, 128),
            held(F32, tiles, 128, width),
            held(BF16, per, ncol, cols_dev, width),
            held(BF16, per, total, width),
            held(BF16, per, total, 3 * width),
            held(F32, per, total, width),
            held(F32, heads * per, total),
            held(BF16, heads * per, total),
            held(BF16, 2, ndev // 2, heads * per, total),
            held(F32, heads, total, total),
            held(BF16, per, total, width),
            held(BF16, per, total, width),
            *sems(ndev), *sems(parts, ndev), *sems(parts, ndev), *sems(per, ncol), *sems(ndev // 2),
            pltpu.SemaphoreType.DMA, pltpu.SemaphoreType.DMA,
            *sems(per, ncol),
        ],
        compiler_params=pltpu.CompilerParams(
            collective_id=0, has_side_effects=True, vmem_limit_bytes=56 * 1024 * 1024
        ),
    )(valid_length, pair, tri_in, tri_gate, tri_out, att_in, att_bias, att_out)


def solution(mesh):
    placed = (P("row", "col", None), P(), P(), P(), P(), P(), P(), P())
    return jax.shard_map(
        per_device, mesh=mesh, in_specs=placed, out_specs=P("row", "col", None), check_vma=False
    )
```

```python
import functools

import jax
import jax.numpy as jnp
from jax import lax
from jax.experimental import pallas as pl
from jax.experimental.pallas import tpu as pltpu
from jax.sharding import PartitionSpec as P

MESH = pl.DeviceIdType.MESH
F32 = jnp.float32
BF16 = jnp.bfloat16


def norm(values, axis):
    center = values - jnp.mean(values, axis=axis, keepdims=True)
    return center * lax.rsqrt(jnp.mean(center * center, axis=axis, keepdims=True) + 1e-05)


def swap_groups(blocks, lane, group):
    count = len(blocks)
    width = count * group
    out = []
    for b in range(count):
        total = None
        for a in range(count):
            shift = (group * (a - b)) % width
            moved = blocks[a] if shift == 0 else pltpu.roll(blocks[a], shift, 1)
            total = moved if total is None else jnp.where(lane == a, moved, total)
        out.append(total)
    return out


def kernel(
    dims,
    valid_ref, pair_ref, tri_in_ref, tri_gate_ref, tri_out_ref, att_in_ref, bias_w_ref, att_out_ref,
    out_ref,
    normed_s, edge_f, left_send, right_send, left_recv, right_recv, left_s, right_s,
    prod_send, prod_recv, prod_f, tri_gate_s, mid_send, mid_recv, qkv_s, gate_s,
    bias_f, bias_send, bias_recv, bias_full, gated_s, gated_recv,
    send_l, recv_l, send_r, recv_r, send_p, recv_p, send_m, recv_m, send_b, recv_b, send_c, recv_c,
    send_g, recv_g,
):
    nrow, ncol, rows_dev, cols_dev, width, heads = dims
    ndev = nrow * ncol
    total = ncol * cols_dev
    group = 128 // cols_dev
    tiles = rows_dev // group
    chans = width // ndev
    parts = 2 if chans % 2 == 0 else 1
    each = chans // parts
    per = rows_dev // ncol
    head_size = width // heads
    my_row, my_col = lax.axis_index("row"), lax.axis_index("col")
    me = my_row * ncol + my_col
    valid = valid_ref[0]

    def other(step):
        peer = lax.rem(me + step, ndev)
        return peer, (peer // ncol, lax.rem(peer, ncol))

    def loop(count, act):
        def run(step, carry):
            act(step)
            return carry

        lax.fori_loop(1, count, run, 0)

    barrier = pltpu.get_barrier_semaphore()
    loop(
        ndev,
        lambda step: pl.semaphore_signal(
            barrier, inc=1, device_id=other(step)[1], device_id_type=MESH
        ),
    )

    lanes = lax.broadcasted_iota(jnp.int32, (1, 128), 1)
    lane_col = my_col * cols_dev + lanes % cols_dev
    lane_row = my_row * rows_dev + (lanes // cols_dev) * tiles

    def edges(side):
        first = 2 * side * width
        for t in range(tiles):
            if side == 0:
                rows = jnp.concatenate([pair_ref[g * tiles + t] for g in range(group)], axis=0)
                normed_s[t] = norm(rows, 1).astype(BF16)
            proj = jnp.dot(
                normed_s[t], tri_in_ref[:, first : first + 2 * width], preferred_element_type=F32
            )
            keep = jnp.where((lane_row + t < valid) & (lane_col < valid), 1.0, 0.0)
            edge = jax.nn.sigmoid(proj[:, :width]) * proj[:, width:]
            edge_f[side, pl.ds(t, width, stride=tiles), :] = jnp.transpose(edge) * keep

    def pack(side, target):
        for c in range(chans):
            target[c] = edge_f[side, pl.ds(c * ndev * tiles, ndev * tiles), :].astype(BF16)

    def share(peer):
        return pl.ds(pl.multiple_of(peer * tiles, tiles), tiles)

    def left_copy(step):
        peer, where = other(step)
        return pltpu.make_async_remote_copy(
            src_ref=left_send.at[:, share(peer), :], dst_ref=left_recv.at[me],
            send_sem=send_l.at[step], recv_sem=recv_l.at[step],
            device_id=where, device_id_type=MESH,
        )

    def right_copy(part, step):
        peer, where = other(step)
        some = pl.ds(part * each, each)
        return pltpu.make_async_remote_copy(
            src_ref=right_send.at[some, share(peer), :], dst_ref=right_recv.at[me, some],
            send_sem=send_r.at[part, step], recv_sem=recv_r.at[part, step],
            device_id=where, device_id_type=MESH,
        )

    edges(0)
    pack(0, left_send)
    pl.semaphore_wait(barrier, ndev - 1)
    loop(ndev, lambda step: left_copy(step).start())
    edges(1)
    pack(1, right_send)
    for part in range(parts):
        loop(ndev, lambda step: right_copy(part, step).start())
    left_recv[me] = left_send[:, share(me), :]
    right_recv[me] = right_send[:, share(me), :]
    for t in range(tiles):
        tri_gate_s[t] = jax.nn.sigmoid(
            jnp.dot(normed_s[t], tri_gate_ref[...], preferred_element_type=F32)
        )
    loop(ndev, lambda step: left_copy(step).wait())

    lane = lax.broadcasted_iota(jnp.int32, (tiles, 128), 1) // cols_dev

    def spread(c, source, operand):
        for r in range(nrow):
            for half in range(ncol // group):
                blocks = [
                    source[r * ncol + half * group + a, c].astype(F32) for a in range(group)
                ]
                for b, piece in enumerate(swap_groups(blocks, lane, cols_dev)):
                    operand[
                        pl.ds(r * rows_dev + b * tiles, tiles), pl.ds(half * 128, 128)
                    ] = piece.astype(BF16)

    def prod_copy(part, step):
        peer, where = other(step)
        some = pl.ds(part * each, each)
        return pltpu.make_async_remote_copy(
            src_ref=prod_send.at[peer, some], dst_ref=prod_recv.at[me, some],
            send_sem=send_p.at[part, step], recv_sem=recv_p.at[part, step],
            device_id=where, device_id_type=MESH,
        )

    for c in range(chans):
        spread(c, left_recv, left_s.at[c])
    for part in range(parts):
        loop(ndev, lambda step: right_copy(part, step).wait())
        for c in range(part * each, (part + 1) * each):
            spread(c, right_recv, right_s.at[c])
            products = lax.dot_general(
                left_s[c], right_s[c], (((1,), (1,)), ((), ())), preferred_element_type=F32
            )
            for r in range(nrow):
                for half in range(ncol // group):
                    blocks = [
                        products[
                            r * rows_dev + a * tiles : r * rows_dev + (a + 1) * tiles,
                            half * 128 : (half + 1) * 128,
                        ]
                        for a in range(group)
                    ]
                    for b, piece in enumerate(swap_groups(blocks, lane, cols_dev)):
                        prod_send[r * ncol + half * group + b, c] = piece.astype(BF16)
        loop(ndev, lambda step: prod_copy(part, step).start())
    prod_recv[me] = prod_send[me]

    for part in range(parts):
        loop(ndev, lambda step: prod_copy(part, step).wait())
        for c in range(part * each, (part + 1) * each):
            for d in range(ndev):
                prod_f[pl.ds((c * ndev + d) * tiles, tiles), :] = prod_recv[d, c].astype(F32)

    def strip(peer):
        return pl.ds(pl.multiple_of(peer * cols_dev, cols_dev), cols_dev)

    def mid_copy(i, step):
        peer = lax.rem(my_col + step, ncol)
        return pltpu.make_async_remote_copy(
            src_ref=mid_send.at[i, peer], dst_ref=mid_recv.at[i, strip(my_col), :],
            send_sem=send_m.at[i, step], recv_sem=recv_m.at[i, step],
            device_id=(my_row, peer), device_id_type=MESH,
        )

    for i in range(per):
        for t in range(i, tiles, per):
            prods = norm(prod_f[pl.ds(t, width, stride=tiles), :], 0)
            prods = jnp.transpose(prods).astype(BF16)
            update = jnp.dot(prods, tri_out_ref[...], preferred_element_type=F32)
            rows = jnp.concatenate([pair_ref[g * tiles + t] for g in range(group)], axis=0)
            middle = rows + tri_gate_s[t] * update
            normed_mid = norm(middle, 1).astype(BF16)
            for g in range(group):
                row = g * tiles + t
                out_ref[row] = middle[g * cols_dev : (g + 1) * cols_dev]
                mid_send[i, row // per] = normed_mid[g * cols_dev : (g + 1) * cols_dev]
        for step in range(1, ncol):
            mid_copy(i, step).start()
        mid_recv[i, strip(my_col), :] = mid_send[i, my_col]

    for i in range(per):
        for step in range(1, ncol):
            mid_copy(i, step).wait()
        own = lax.dot_general(
            bias_w_ref[...], mid_recv[i], (((1,), (1,)), ((), ())), preferred_element_type=F32
        )
        for h in range(heads):
            bias_f[pl.ds(h * per + i, 1), :] = own[h : h + 1]
        if i < per - 1:
            project(i, mid_recv, att_in_ref, qkv_s, gate_s, width, head_size)
    bias_send[...] = bias_f[...].astype(BF16)

    side = lax.rem(my_col, 2)
    mine = me // 2

    def bias_copy(step):
        peer = 2 * lax.rem(mine + step, ndev // 2) + side
        return pltpu.make_async_remote_copy(
            src_ref=bias_send, dst_ref=bias_recv.at[side, mine],
            send_sem=send_b.at[step], recv_sem=recv_b.at[step],
            device_id=(peer // ncol, lax.rem(peer, ncol)), device_id_type=MESH,
        )

    loop(ndev // 2, lambda step: bias_copy(step).start())
    bias_recv[side, mine] = bias_send[...]
    project(per - 1, mid_recv, att_in_ref, qkv_s, gate_s, width, head_size)
    loop(ndev // 2, lambda step: bias_copy(step).wait())
    hand = pltpu.make_async_remote_copy(
        src_ref=bias_recv.at[side], dst_ref=bias_recv.at[side],
        send_sem=send_c, recv_sem=recv_c,
        device_id=(my_row, my_col + 1 - 2 * side), device_id_type=MESH,
    )
    hand.start()
    hand.wait()
    tokens = lax.broadcasted_iota(jnp.int32, (1, total), 1)
    mask = jnp.where(tokens < valid, 0.0, -1000000000.0)
    for d in range(ndev):
        piece = bias_recv[d % 2, d // 2].astype(F32) + mask
        for h in range(heads):
            bias_full[h, pl.ds(d * per, per), :] = piece[h * per : (h + 1) * per]

    block = 128
    head = lax.broadcasted_iota(jnp.int32, (block, width), 1) // head_size

    def home_copy(i, step):
        peer = lax.rem(my_col + step, ncol)
        return pltpu.make_async_remote_copy(
            src_ref=gated_s.at[i, strip(peer), :], dst_ref=gated_recv.at[i, strip(my_col), :],
            send_sem=send_g.at[i, step], recv_sem=recv_g.at[i, step],
            device_id=(my_row, peer), device_id_type=MESH,
        )

    def attend(i, carry):
        keys = qkv_s[i, :, width : 2 * width]
        values = jnp.concatenate(
            [qkv_s[i, :, 2 * width : 3 * width], jnp.ones((total, width), BF16)], axis=1
        )
        for first in range(0, total, block):
            query = qkv_s[i, first : first + block, :width]
            top = jnp.zeros((block, width), F32)
            bottom = jnp.ones((block, width), F32)
            for h in range(heads):
                scores = lax.dot_general(
                    jnp.where(head == h, query, jnp.zeros_like(query)), keys,
                    (((1,), (1,)), ((), ())), preferred_element_type=F32,
                )
                scores = scores + bias_full[h, first : first + block, :]
                expo = jnp.exp(scores - jnp.max(scores, axis=1, keepdims=True)).astype(BF16)
                both = jnp.dot(expo, values, preferred_element_type=F32)
                top = jnp.where(head == h, both[:, :width], top)
                bottom = jnp.where(head == h, both[:, width:], bottom)
            gated_s[i, first : first + block, :] = (
                gate_s[i, first : first + block, :] * top / bottom
            ).astype(BF16)
        for step in range(1, ncol):
            home_copy(i, step).start()
        gated_recv[i, strip(my_col), :] = gated_s[i, strip(my_col), :]
        return carry

    lax.fori_loop(0, per, attend, 0)

    def finish(i, carry):
        for step in range(1, ncol):
            home_copy(i, step).wait()
        added = jnp.dot(gated_recv[i], att_out_ref[...], preferred_element_type=F32)
        for q in range(ncol):
            out_ref[q * per + i] += added[q * cols_dev : (q + 1) * cols_dev]
        return carry

    lax.fori_loop(0, per, finish, 0)


def project(i, mid_recv, att_in_ref, qkv_s, gate_s, width, head_size):
    proj = jnp.dot(mid_recv[i], att_in_ref[...], preferred_element_type=F32)
    qkv_s[i, :, :width] = (proj[:, :width] * head_size ** (-0.5)).astype(BF16)
    qkv_s[i, :, width : 3 * width] = proj[:, width : 3 * width].astype(BF16)
    gate_s[i] = jax.nn.sigmoid(proj[:, 3 * width :])


def per_device(pair, valid_length, tri_in, tri_gate, tri_out, att_in, att_bias, att_out):
    rows_dev, cols_dev, width = pair.shape
    heads = att_bias.shape[1]
    nrow, ncol = lax.axis_size("row"), lax.axis_size("col")
    ndev = nrow * ncol
    total = ncol * cols_dev
    tiles = rows_dev // (128 // cols_dev)
    chans = width // ndev
    parts = 2 if chans % 2 == 0 else 1
    per = rows_dev // ncol
    vmem = pl.BlockSpec(memory_space=pltpu.VMEM)
    sems = lambda *shape: [pltpu.SemaphoreType.DMA(shape)] * 2
    held = lambda dtype, *shape: pltpu.VMEM(shape, dtype)
    return pl.pallas_call(
        functools.partial(kernel, (nrow, ncol, rows_dev, cols_dev, width, heads)),
        out_shape=jax.ShapeDtypeStruct((rows_dev, cols_dev, width), F32),
        in_specs=[pl.BlockSpec(memory_space=pltpu.SMEM)] + [vmem] * 7,
        out_specs=vmem,
        scratch_shapes=[
            held(BF16, tiles, 128, width),
            held(F32, 2, width * tiles, 128),
            held(BF16, chans, ndev * tiles, 128),
            held(BF16, chans, ndev * tiles, 128),
            held(BF16, ndev, chans, tiles, 128),
            held(BF16, ndev, chans, tiles, 128),
            held(BF16, chans, total, total),
            held(BF16, chans, total, total),
            held(BF16, ndev, chans, tiles, 128),
            held(BF16, ndev, chans, tiles, 128),
            held(F32, width * tiles, 128),
            held(F32, tiles, 128, width),
            held(BF16, per, ncol, cols_dev, width),
            held(BF16, per, total, width),
            held(BF16, per, total, 3 * width),
            held(F32, per, total, width),
            held(F32, heads * per, total),
            held(BF16, heads * per, total),
            held(BF16, 2, ndev // 2, heads * per, total),
            held(F32, heads, total, total),
            held(BF16, per, total, width),
            held(BF16, per, total, width),
            *sems(ndev), *sems(parts, ndev), *sems(parts, ndev), *sems(per, ncol), *sems(ndev // 2),
            pltpu.SemaphoreType.DMA, pltpu.SemaphoreType.DMA,
            *sems(per, ncol),
        ],
        compiler_params=pltpu.CompilerParams(
            collective_id=0, has_side_effects=True, vmem_limit_bytes=56 * 1024 * 1024
        ),
    )(valid_length, pair, tri_in, tri_gate, tri_out, att_in, att_bias.T, att_out)


def solution(mesh):
    placed = (P("row", "col", None), P(), P(), P(), P(), P(), P(), P())
    return jax.shard_map(
        per_device, mesh=mesh, in_specs=placed, out_specs=P("row", "col", None), check_vma=False
    )
```
